32 devices in a mesh: region: 8 (over z, x), member: 4 (over y, core).
Axes of the slice: x: 2, y: 2, z: 4, core: 2. Of those that a mesh axis runs over, the one named last changes fastest.
Arguments:
- members: float32 [256, 128, 1024], P('member', 'region'), may hold values from -6 to 6
- obs_value: float32 [128, 1024], P('region'), may hold values from -6 to 6
- obs_precision: float32 [128, 1024], P('region'), may hold values from 0.02 to 200
- obs_index: int32 [128, 1024], P('region'), may hold values from 0 to 1023, as said below
- obs_count: int32 [128], P('region'), may hold values from 256 to 1024
Outputs:
- analysis: float32 [256, 128, 1024], P('member', 'region')
The draws below stay inside these ranges and needn't reach their ends.
Inputs may be any that keep to these rules, and one draw needn't show every extreme that they name: `obs_count`: slots of a tile from its count onward are empty. `obs_index`: position within its own tile.
All inputs are finite; a program needn't handle non-finite values.
Results may differ from the reference program's by a relative error of at most 0.0005.
Values sent between devices are 32-bit elements; how exact they have to be, the bound alone decides.
A program may use at most 64 MiB of HBM per device.

```python
import math
import jax
import jax.numpy as jnp
from jax import lax

K = 256
TILE = 1024
OBS = 1024
TILES_DEV = 16
ITERS = 12
TILES = 128
N_REGION = 8


def draw_obs_index(key, part):
    hot_key = jax.random.fold_in(key, 11)
    pick_key = jax.random.fold_in(key, 12)
    wide_key = jax.random.fold_in(key, 13)
    centres = jax.random.randint(hot_key, (TILES, 4), 0, TILE, dtype=jnp.int32)
    selector = jax.random.randint(pick_key, (TILES, OBS), 0, 4, dtype=jnp.int32)
    spread = jax.random.randint(wide_key, (TILES, OBS), 0, TILE, dtype=jnp.int32)
    repeated = jnp.take_along_axis(centres, selector, axis=1)
    slot_ids = jnp.arange(OBS, dtype=jnp.int32)[None, :]
    return jnp.where(slot_ids < OBS // 8, repeated, spread).astype(jnp.int32)


def draw_obs_precision(key, part):
    low_key = jax.random.fold_in(key, 21)
    high_key = jax.random.fold_in(key, 22)
    background = jnp.exp(jax.random.uniform(low_key, (TILES, OBS), jnp.float32, math.log(0.02), math.log(2.0)))
    background = jnp.clip(background, 0.02, 2.0)
    precise = jnp.exp(jax.random.uniform(high_key, (TILES, OBS), jnp.float32, math.log(40.0), math.log(200.0)))
    precise = jnp.clip(precise, 40.0, 200.0)
    slot_ids = jnp.arange(OBS, dtype=jnp.int32)[None, :]
    return jnp.where(slot_ids < OBS // 8, precise, background).astype(jnp.float32)


def place_ends(values, stream_key, low, largest):
    spot = [jax.random.randint(jax.random.fold_in(stream_key, axis), (), 0, length) for axis, length in enumerate(values.shape)]
    main_axis = values.shape.index(max(values.shape))
    beside = spot[:main_axis] + [(spot[main_axis] + 1) % values.shape[main_axis]] + spot[main_axis + 1:]
    return values.at[tuple(spot)].set(low).at[tuple(beside)].set(largest)


def block_scale(key, shape, cuts, smallest, largest):
    loudness, own = 1.0, jax.random.fold_in(key, 6)
    for dim, shards_of in cuts:
        draws = jnp.exp(jax.random.uniform(jax.random.fold_in(own, dim), (shards_of,), jnp.float32, smallest / len(cuts), largest / len(cuts)))
        loudness = loudness * jnp.repeat(draws, shape[dim] // shards_of).reshape([-1 if axis == dim else 1 for axis in range(len(shape))])
    return loudness


def gaussian(key, dims, scale, most, cuts=(), held_as=jnp.bfloat16):
    values = scale * jax.random.normal(key, dims, jnp.float32)
    if cuts:
        values = values * block_scale(key, dims, cuts, -0.22, 0.18)
    return jnp.clip(values, -most, most).astype(held_as)


def setup_inputs(seed: int = 0) -> dict:
    keys = jax.random.split(jax.random.key(seed), 6)
    members = gaussian(keys[0], (K, TILES, TILE), 1.0, 6.0, ((0, 4), (1, 8)), jnp.float32)
    obs_value = gaussian(keys[1], (TILES, OBS), 1.0, 6.0, ((0, 8),), jnp.float32)
    obs_precision = draw_obs_precision(jax.random.fold_in(keys[5], 71), 0)
    obs_index = draw_obs_index(jax.random.fold_in(keys[5], 71), 0)
    obs_count = place_ends(jax.random.randint(keys[4], (TILES,), OBS // 4, OBS + 1), jax.random.fold_in(keys[4], 1), OBS // 4, OBS).astype(jnp.int32)
    return dict(members=members, obs_value=obs_value, obs_precision=obs_precision, obs_index=obs_index, obs_count=obs_count)


def observe(states, places, observed, accuracy, filled):
    average = lax.optimization_barrier(jnp.sum(states, axis=0)) / K
    deviation = states - average[None]
    sampled = jnp.take_along_axis(deviation, places[None], axis=2)
    baseline = jnp.take_along_axis(average, places, axis=1)
    slot_ids = jnp.arange(places.shape[1], dtype=jnp.int32)
    active = slot_ids[None, :] < filled[:, None]
    weight_root = jnp.where(active, jnp.sqrt(accuracy), jnp.float32(0.0))
    scaled = sampled * weight_root[None]
    innov_row = (weight_root * (observed - baseline))[None]
    stacked = jnp.concatenate([scaled, innov_row], axis=0)
    return (average, deviation, stacked)

def outer_gram(stacked):
    return jnp.einsum('ibo,jbo->bij', stacked, stacked, precision=lax.Precision.HIGHEST)

def transform_weights(gram_matrix):
    ensemble = gram_matrix.shape[1] - 1
    identity = jnp.eye(ensemble, dtype=jnp.float32)
    system = (ensemble - 1.0) * identity + gram_matrix[:, :ensemble, :ensemble]
    right_side = gram_matrix[:, :ensemble, ensemble]
    factor = jnp.sqrt(lax.optimization_barrier(jnp.sum(system * system, axis=(1, 2))) + 1e-06)
    root_iter = system / factor[:, None, None]
    inverse_iter = jnp.broadcast_to(identity, system.shape)

    def one_sweep(sweep_no, iterates):
        root_now, inverse_now = iterates
        middle = 3.0 * identity - jnp.einsum('bij,bjk->bik', inverse_now, root_now, precision=lax.Precision.HIGHEST)
        root_next = 0.5 * jnp.einsum('bij,bjk->bik', root_now, middle, precision=lax.Precision.HIGHEST)
        inverse_next = 0.5 * jnp.einsum('bij,bjk->bik', middle, inverse_now, precision=lax.Precision.HIGHEST)
        return (root_next, inverse_next)
    root_iter, inverse_iter = lax.fori_loop(0, ITERS, one_sweep, (root_iter, inverse_iter))
    inverse_root = inverse_iter / jnp.sqrt(factor)[:, None, None]
    pulled = jnp.einsum('bij,bj->bi', inverse_root, right_side, precision=lax.Precision.HIGHEST)
    shifted = jnp.einsum('bij,bj->bi', inverse_root, pulled, precision=lax.Precision.HIGHEST)
    return math.sqrt(ensemble - 1.0) * inverse_root + shifted[:, :, None]

def analyse(average, deviation, gram_matrix):
    weights = transform_weights(gram_matrix)
    return average[None] + jnp.einsum('jbc,bjk->kbc', deviation, weights, precision=lax.Precision.HIGHEST)

def reference(members, obs_value, obs_precision, obs_index, obs_count):
    columns = members.reshape(K, N_REGION, TILES_DEV, TILE).transpose(1, 0, 2, 3)
    obs_values = obs_value.reshape(N_REGION, TILES_DEV, OBS)
    accuracies = obs_precision.reshape(N_REGION, TILES_DEV, OBS)
    indices = obs_index.reshape(N_REGION, TILES_DEV, OBS)
    obs_counts = obs_count.reshape(N_REGION, TILES_DEV)

    def gram_of(entries):
        states, places, observed, accuracy, filled = entries
        return outer_gram(observe(states, places, observed, accuracy, filled)[2])
    gram_tiles = lax.map(gram_of, (columns, indices, obs_values, accuracies, obs_counts))
    combined = gram_tiles + 0.5 * (jnp.roll(gram_tiles, 1, axis=0) + jnp.roll(gram_tiles, -1, axis=0))

    def analyse_column(entries):
        states, places, observed, accuracy, filled, gram_matrix = entries
        average, deviation, stacked = observe(states, places, observed, accuracy, filled)
        return analyse(average, deviation, gram_matrix)
    result = lax.map(analyse_column, (columns, indices, obs_values, accuracies, obs_counts, combined))
    return result.transpose(1, 0, 2, 3).reshape(K, N_REGION * TILES_DEV, TILE)
```

```python
import functools
import math

import jax
import jax.numpy as jnp
from jax import lax
from jax.experimental import pallas as pl
from jax.experimental.pallas import tpu as pltpu
from jax.sharding import PartitionSpec as P

ITERS = 12
LANES = 128
MESH = pl.DeviceIdType.MESH
F32 = jnp.float32
BF16 = jnp.bfloat16


def split3(x):
    a = x.astype(BF16)
    rest = x - a.astype(F32)
    b = rest.astype(BF16)
    return a, b, (rest - b.astype(F32)).astype(BF16)


def dot(a, b):
    return jnp.dot(a, b, preferred_element_type=F32)


def dot_nt(a, b):
    return lax.dot_general(a, b, (((1,), (1,)), ((), ())), preferred_element_type=F32)


def product(a, b):
    a1, a2, a3 = a
    b1, b2, b3 = b
    left = jnp.concatenate([a1, a3, a2, a1, a2, a1], axis=1)
    right = jnp.concatenate([b3, b1, b2, b2, b1, b1], axis=0)
    return dot(left, right)


def gram(states, places, exact, observed):
    size, width = states.shape
    half = size // 2
    groups = width // LANES
    slots = places.shape[1]

    high = lax.shift_right_logical(places, 7)
    low = lax.bitwise_and(places, LANES - 1)
    rows = lax.broadcasted_iota(jnp.int32, (groups, slots), 0) == high
    both = jnp.concatenate(
        [jnp.where(rows, exact, 0.0), jnp.where(rows, exact * observed, 0.0)], axis=0
    )
    one_hot = jnp.where(
        lax.broadcasted_iota(jnp.int32, (LANES, slots), 0) == low, 1.0, 0.0
    ).astype(BF16)
    e1, e2, e3 = split3(both)
    sums = dot_nt(e3, one_hot) + dot_nt(e2, one_hot) + dot_nt(e1, one_hot)
    c = jnp.concatenate([sums[i : i + 1] for i in range(groups)], axis=1)
    d = jnp.concatenate([sums[groups + i : groups + i + 1] for i in range(groups)], axis=1)

    average = jnp.sum(states, axis=0, keepdims=True) / size
    deviation = states - average
    s1, s2, s3 = split3(deviation * jnp.sqrt(c))
    cross = dot_nt(s1, s3) + dot_nt(s1, s2)
    own = (dot_nt(s2, s2) + (cross + cross.T)) + dot_nt(s1, s1)

    pulled = deviation * (d - c * average)
    folded = pulled[:, :LANES]
    for i in range(1, groups):
        folded = folded + pulled[:, i * LANES : (i + 1) * LANES]
    right = jnp.sum(folded.T, axis=0, keepdims=True)

    row = lax.broadcasted_iota(jnp.int32, (half, half), 0)
    col = lax.broadcasted_iota(jnp.int32, (half, half), 1)
    first, last = own[:half, :half], own[half:, half:]
    diagonal = jnp.sum(jnp.where(row == col, last, 0.0), axis=0, keepdims=True)
    square = jnp.concatenate([own[:half, half:], jnp.where(row <= col, first, last)], axis=1)
    tail = jnp.concatenate([right, jnp.concatenate([diagonal, diagonal], axis=1)], axis=0)
    return square, jnp.concatenate([tail, jnp.zeros((6, size), F32)], axis=0)


def unpack(packed, size):
    half = size // 2
    row = lax.broadcasted_iota(jnp.int32, (half, half), 0)
    col = lax.broadcasted_iota(jnp.int32, (half, half), 1)
    upper, mixed = packed[:half, :half], packed[:half, half:]
    right = packed[half : half + 1]
    diagonal = packed[half + 1 : half + 2, :half]
    turned = mixed.T
    first = jnp.where(row <= col, mixed, turned)
    last = jnp.where(row > col, mixed, turned)
    last = jnp.where(row == col, diagonal, last)
    full = jnp.concatenate(
        [
            jnp.concatenate([first, upper], axis=1),
            jnp.concatenate([upper.T, last], axis=1),
        ],
        axis=0,
    )
    return full, right


def identity_of(size):
    row = lax.broadcasted_iota(jnp.int32, (size, size), 0)
    col = lax.broadcasted_iota(jnp.int32, (size, size), 1)
    return jnp.where(row == col, 1.0, 0.0).astype(F32)


def growth(u, z, size):
    identity = identity_of(size)
    x = split3(u if z is None else product(z, u))
    plain = u if z is None else x[0].astype(F32) + x[1].astype(F32) + x[2].astype(F32)
    squared = product(x, x)
    inner = (1 / 16) * squared - (9 / 16) * plain
    outer = product(split3(squared), split3(inner))
    return (36 / 16) * identity - (39 / 16) * plain + (27 / 16) * squared + outer


def kernel(
    count, columns,
    x_hbm, value_ref, precision_ref, index_ref, filled_ref, out_ref,
    x_ref, send_ref, got_ref, own_ref, west_ref, east_ref, result_ref,
    u_ref, z_ref, right_ref, scale_ref,
    x_sem, in_send, in_recv, gram_send, gram_recv, out_send, out_recv, out_local,
):
    me, column = lax.axis_index("member"), lax.axis_index("region")
    owned, size, width = got_ref.shape
    tiles = owned * count
    rows = size // count
    slots = index_ref.shape[1]
    half = size // 2

    def peer(k):
        return lax.rem(me + k, count)

    x_copy = pltpu.make_async_copy(x_hbm, x_ref, x_sem)
    x_copy.start()
    beside = (lax.rem(column + 1, columns), lax.rem(column + columns - 1, columns))
    barrier = pltpu.get_barrier_semaphore()
    for k in range(1, count):
        pl.semaphore_signal(barrier, inc=1, device_id={"member": peer(k)}, device_id_type=MESH)
    for b in beside:
        pl.semaphore_signal(barrier, inc=1, device_id={"region": b}, device_id_type=MESH)
    pl.semaphore_wait(barrier, count + 1)

    def in_copy(j, k):
        return pltpu.make_async_remote_copy(
            src_ref=send_ref.at[j, peer(k)],
            dst_ref=got_ref.at[j, pl.ds(pl.multiple_of(me * rows, rows), rows)],
            send_sem=in_send.at[j, k - 1],
            recv_sem=in_recv.at[j, k - 1],
            device_id={"member": peer(k)},
            device_id_type=MESH,
        )

    def out_copy(j, k):
        return pltpu.make_async_remote_copy(
            src_ref=result_ref.at[j, pl.ds(pl.multiple_of(peer(k) * rows, rows), rows)],
            dst_ref=out_ref.at[j * count + me],
            send_sem=out_send.at[j, k - 1],
            recv_sem=out_recv.at[j, k - 1],
            device_id={"member": peer(k)},
            device_id_type=MESH,
        )

    def gram_copy(j, side):
        return pltpu.make_async_remote_copy(
            src_ref=own_ref.at[j],
            dst_ref=(west_ref, east_ref)[side].at[j],
            send_sem=gram_send.at[j, side],
            recv_sem=gram_recv.at[j, side],
            device_id={"region": beside[side]},
            device_id_type=MESH,
        )

    x_copy.wait()

    def scatter(j, carry):
        for q in range(count):
            send_ref[j, q] = x_ref[:, j * count + q, :]
        for k in range(1, count):
            in_copy(j, k).start()
        got_ref[j, pl.ds(pl.multiple_of(me * rows, rows), rows)] = send_ref[j, me]
        return carry

    lax.fori_loop(0, owned, scatter, 0)

    def make_gram(j):
        for k in range(1, count):
            in_copy(j, k).wait_recv()
        t = j * count + me
        slot = lax.broadcasted_iota(jnp.int32, (1, slots), 1)
        exact = jnp.where(slot < filled_ref[t], precision_ref[pl.ds(t, 1), :], 0.0)
        square, tail = gram(
            got_ref[j], index_ref[pl.ds(t, 1), :], exact, value_ref[pl.ds(t, 1), :]
        )
        own_ref[j, :half] = square
        own_ref[j, half:] = tail
        for side in range(2):
            gram_copy(j, side).start()

    def two_steps(_, carry):
        u, z = split3(u_ref[...]), split3(z_ref[...])
        g = split3(growth(u, z, size))
        u_ref[...] = product(u, g)
        z_ref[...] = product(g, z)
        return carry

    make_gram(0)
    loops = ITERS // 2 - 2

    def analyse(j, carry):
        for side in range(2):
            gram_copy(j, side).wait_recv()
        full, right = unpack(own_ref[j] + 0.5 * (west_ref[j] + east_ref[j]), size)
        system = (size - 1.0) * identity_of(size) + full
        total = jnp.sum(jnp.sum(system * system, axis=0, keepdims=True), axis=1, keepdims=True)
        scale = jnp.sqrt(total + 1e-6)
        right_ref[...] = right
        scale_ref[...] = jnp.broadcast_to(scale, (1, LANES))
        u = system / scale
        g = growth(u, None, size)
        z_ref[...] = g
        u_ref[...] = product(split3(u), split3(g))
        lax.fori_loop(0, loops // 2, two_steps, 0)

        @pl.when(j + 1 < owned)
        def _():
            make_gram(j + 1)

        lax.fori_loop(loops // 2, loops, two_steps, 0)
        u, z = split3(u_ref[...]), split3(z_ref[...])
        inverse = product(split3(growth(u, z, size)), z) / jnp.sqrt(scale_ref[:, :1])
        pulled = jnp.sum(inverse * right_ref[...], axis=1, keepdims=True)
        shift = jnp.sum(inverse * pulled, axis=0, keepdims=True)
        weights = math.sqrt(size - 1.0) * inverse + shift
        states = got_ref[j]
        average = jnp.sum(states, axis=0, keepdims=True) / size
        w1, w2, _ = split3(weights)
        d1, d2, _ = split3(states - average)
        left = jnp.concatenate([w2, w1, w1], axis=1)
        right = jnp.concatenate([d1, d2, d1], axis=0)
        result_ref[j] = average + dot(left, right)
        for k in range(1, count):
            out_copy(j, k).start()
        pltpu.make_async_copy(
            result_ref.at[j, pl.ds(pl.multiple_of(me * rows, rows), rows)],
            out_ref.at[j * count + me],
            out_local.at[j],
        ).start()
        return carry

    lax.fori_loop(0, owned, analyse, 0)

    def finish(j, carry):
        for k in range(1, count):
            in_copy(j, k).wait_send()
            out_copy(j, k).wait()
        for side in range(2):
            gram_copy(j, side).wait_send()
        pltpu.make_async_copy(
            result_ref.at[j, pl.ds(pl.multiple_of(me * rows, rows), rows)],
            out_ref.at[j * count + me],
            out_local.at[j],
        ).wait()
        return carry

    lax.fori_loop(0, owned, finish, 0)


def shards(members, obs_value, obs_precision, obs_index, obs_count):
    count, columns = lax.axis_size("member"), lax.axis_size("region")
    rows, tiles, width = members.shape
    owned = tiles // count
    size = count * rows
    packed = pltpu.VMEM((owned, size // 2 + 8, size), F32)
    whole = pl.BlockSpec(memory_space=pltpu.VMEM)
    anywhere = pl.BlockSpec(memory_space=pl.ANY)
    dma = pltpu.SemaphoreType.DMA
    out = pl.pallas_call(
        functools.partial(kernel, count, columns),
        in_specs=[anywhere, whole, whole, whole, pl.BlockSpec(memory_space=pltpu.SMEM)],
        out_specs=anywhere,
        out_shape=jax.ShapeDtypeStruct((tiles, rows, width), F32),
        scratch_shapes=[
            pltpu.VMEM((rows, tiles, width), F32),
            pltpu.VMEM((owned, count, rows, width), F32),
            pltpu.VMEM((owned, size, width), F32),
            packed, packed, packed,
            pltpu.VMEM((owned, size, width), F32),
            pltpu.VMEM((size, size), F32),
            pltpu.VMEM((size, size), F32),
            pltpu.VMEM((1, size), F32),
            pltpu.VMEM((1, LANES), F32),
            dma,
            dma((owned, count - 1)),
            dma((owned, count - 1)),
            dma((owned, 2)),
            dma((owned, 2)),
            dma((owned, count - 1)),
            dma((owned, count - 1)),
            dma((owned,)),
        ],
        compiler_params=pltpu.CompilerParams(
            collective_id=0, has_side_effects=True, vmem_limit_bytes=60 * 2**20
        ),
    )(members, obs_value, obs_precision, obs_index, obs_count)
    return out.transpose(1, 0, 2)


def solution(mesh):
    in_specs = (
        P("member", "region", None),
        P("region", None),
        P("region", None),
        P("region", None),
        P("region"),
    )
    return jax.shard_map(
        shards,
        mesh=mesh,
        in_specs=in_specs,
        out_specs=P("member", "region", None),
        check_vma=False,
    )
```

```python
import functools
import math

import jax
import jax.numpy as jnp
from jax import lax
from jax.experimental import pallas as pl
from jax.experimental.pallas import tpu as pltpu
from jax.sharding import PartitionSpec as P

ITERS = 12
LANES = 128
MESH = pl.DeviceIdType.MESH
F32 = jnp.float32
BF16 = jnp.bfloat16


def split3(x):
    a = x.astype(BF16)
    rest = x - a.astype(F32)
    b = rest.astype(BF16)
    return a, b, (rest - b.astype(F32)).astype(BF16)


def dot(a, b):
    return jnp.dot(a, b, preferred_element_type=F32)


def dot_nt(a, b):
    return lax.dot_general(a, b, (((1,), (1,)), ((), ())), preferred_element_type=F32)


def product(a, b):
    a1, a2, a3 = a
    b1, b2, b3 = b
    left = jnp.concatenate([a1, a3, a2, a1, a2, a1], axis=1)
    right = jnp.concatenate([b3, b1, b2, b2, b1, b1], axis=0)
    return dot(left, right)


def gram(states, places, exact, observed):
    size, width = states.shape
    half = size // 2
    groups = width // LANES
    slots = places.shape[1]

    high = lax.shift_right_logical(places, 7)
    low = lax.bitwise_and(places, LANES - 1)
    rows = lax.broadcasted_iota(jnp.int32, (groups, slots), 0) == high
    both = jnp.concatenate(
        [jnp.where(rows, exact, 0.0), jnp.where(rows, exact * observed, 0.0)], axis=0
    )
    one_hot = jnp.where(
        lax.broadcasted_iota(jnp.int32, (LANES, slots), 0) == low, 1.0, 0.0
    ).astype(BF16)
    e1, e2, e3 = split3(both)
    sums = dot_nt(e3, one_hot) + dot_nt(e2, one_hot) + dot_nt(e1, one_hot)
    c = jnp.concatenate([sums[i : i + 1] for i in range(groups)], axis=1)
    d = jnp.concatenate([sums[groups + i : groups + i + 1] for i in range(groups)], axis=1)

    average = jnp.sum(states, axis=0, keepdims=True) / size
    deviation = states - average
    s1, s2, s3 = split3(deviation * jnp.sqrt(c))
    cross = dot_nt(s1, s3) + dot_nt(s1, s2)
    own = (dot_nt(s2, s2) + (cross + cross.T)) + dot_nt(s1, s1)

    pulled = deviation * (d - c * average)
    folded = pulled[:, :LANES]
    for i in range(1, groups):
        folded = folded + pulled[:, i * LANES : (i + 1) * LANES]
    right = jnp.sum(folded.T, axis=0, keepdims=True)

    row = lax.broadcasted_iota(jnp.int32, (half, half), 0)
    col = lax.broadcasted_iota(jnp.int32, (half, half), 1)
    first, last = own[:half, :half], own[half:, half:]
    diagonal = jnp.sum(jnp.where(row == col, last, 0.0), axis=0, keepdims=True)
    square = jnp.concatenate([own[:half, half:], jnp.where(row <= col, first, last)], axis=1)
    tail = jnp.concatenate([right, jnp.concatenate([diagonal, diagonal], axis=1)], axis=0)
    return square, jnp.concatenate([tail, jnp.zeros((6, size), F32)], axis=0)


def unpack(packed, size):
    half = size // 2
    row = lax.broadcasted_iota(jnp.int32, (half, half), 0)
    col = lax.broadcasted_iota(jnp.int32, (half, half), 1)
    upper, mixed = packed[:half, :half], packed[:half, half:]
    right = packed[half : half + 1]
    diagonal = packed[half + 1 : half + 2, :half]
    turned = mixed.T
    first = jnp.where(row <= col, mixed, turned)
    last = jnp.where(row > col, mixed, turned)
    last = jnp.where(row == col, diagonal, last)
    full = jnp.concatenate(
        [
            jnp.concatenate([first, upper], axis=1),
            jnp.concatenate([upper.T, last], axis=1),
        ],
        axis=0,
    )
    return full, right


def identity_of(size):
    row = lax.broadcasted_iota(jnp.int32, (size, size), 0)
    col = lax.broadcasted_iota(jnp.int32, (size, size), 1)
    return jnp.where(row == col, 1.0, 0.0).astype(F32)


def growth(u, z, size):
    identity = identity_of(size)
    x = split3(u if z is None else product(z, u))
    plain = u if z is None else x[0].astype(F32) + x[1].astype(F32) + x[2].astype(F32)
    squared = product(x, x)
    inner = (1 / 16) * squared - (9 / 16) * plain
    outer = product(split3(squared), split3(inner))
    return (36 / 16) * identity - (39 / 16) * plain + (27 / 16) * squared + outer


def kernel(
    count, columns,
    x_hbm, value_hbm, precision_hbm, index_hbm, filled_hbm, out_ref,
    value_ref, precision_ref, index_ref, filled_ref, got_ref, own_ref, west_ref, east_ref, result_ref,
    u_ref, z_ref, right_ref, scale_ref,
    x_sem, table_sem, go_sem, open_sem, in_send, in_recv, gram_send, gram_recv, out_send, out_recv,
):
    me, column = lax.axis_index("member"), lax.axis_index("region")
    owned, size, width = got_ref.shape
    tiles = owned * count
    rows = size // count
    slots = index_ref.shape[1]
    half = size // 2

    def peer(k):
        return lax.rem(me + k, count)

    def own_copy(j):
        return pltpu.make_async_copy(
            x_hbm.at[:, j * count + me, :],
            got_ref.at[j, pl.ds(pl.multiple_of(me * rows, rows), rows)],
            x_sem.at[j],
        )

    tables = (
        (value_hbm, value_ref),
        (precision_hbm, precision_ref),
        (index_hbm, index_ref),
        (filled_hbm, filled_ref),
    )
    table_copies = [
        pltpu.make_async_copy(a, b, table_sem.at[i]) for i, (a, b) in enumerate(tables)
    ]
    for copy in table_copies:
        copy.start()

    beside = (lax.rem(column + 1, columns), lax.rem(column + columns - 1, columns))
    barrier = pltpu.get_barrier_semaphore()
    staggered = count % 2 == 0 and columns % 2 == 0
    free = lax.rem(column + me, 2) == 0
    partner = me + 1 - 2 * lax.rem(me, 2)

    def greet(semaphore):
        for b in beside:
            pl.semaphore_signal(semaphore, inc=1, device_id={"region": b}, device_id_type=MESH)

    for k in range(1, count):
        pl.semaphore_signal(barrier, inc=1, device_id={"member": peer(k)}, device_id_type=MESH)
    if staggered:

        @pl.when(free)
        def _():
            pl.semaphore_wait(barrier, count - 1)
            pl.semaphore_signal(
                go_sem, inc=1, device_id={"member": partner}, device_id_type=MESH
            )
            greet(barrier)

        @pl.when(jnp.logical_not(free))
        def _():
            pl.semaphore_wait(go_sem, 1)

    else:
        greet(barrier)
        pl.semaphore_wait(barrier, count + 1)

    def meet_region():
        if staggered:

            @pl.when(free)
            def _():
                pl.semaphore_wait(open_sem, 2)

            @pl.when(jnp.logical_not(free))
            def _():
                pl.semaphore_wait(barrier, count + 1)
                greet(open_sem)

    def in_copy(j, k):
        return pltpu.make_async_remote_copy(
            src_ref=x_hbm.at[:, j * count + peer(k), :],
            dst_ref=got_ref.at[j, pl.ds(pl.multiple_of(me * rows, rows), rows)],
            send_sem=in_send.at[j, k - 1],
            recv_sem=in_recv.at[j, k - 1],
            device_id={"member": peer(k)},
            device_id_type=MESH,
        )

    def out_copy(j, k):
        return pltpu.make_async_remote_copy(
            src_ref=result_ref.at[j, pl.ds(pl.multiple_of(peer(k) * rows, rows), rows)],
            dst_ref=out_ref.at[:, j * count + me, :],
            send_sem=out_send.at[j, k - 1],
            recv_sem=out_recv.at[j, k - 1],
            device_id={"member": peer(k)},
            device_id_type=MESH,
        )

    def gram_copy(j, side):
        return pltpu.make_async_remote_copy(
            src_ref=own_ref.at[j],
            dst_ref=(west_ref, east_ref)[side].at[j],
            send_sem=gram_send.at[j, side],
            recv_sem=gram_recv.at[j, side],
            device_id={"region": beside[side]},
            device_id_type=MESH,
        )

    for j in range(owned):
        for k in range(1, count):
            in_copy(j, k).start()
    for j in range(owned):
        own_copy(j).start()
    for copy in table_copies:
        copy.wait()
    meet_region()

    def make_gram(j):
        own_copy(j).wait()
        for k in range(1, count):
            in_copy(j, k).wait_recv()
        t = j * count + me
        slot = lax.broadcasted_iota(jnp.int32, (1, slots), 1)
        exact = jnp.where(slot < filled_ref[t], precision_ref[pl.ds(t, 1), :], 0.0)
        square, tail = gram(
            got_ref[j], index_ref[pl.ds(t, 1), :], exact, value_ref[pl.ds(t, 1), :]
        )
        own_ref[j, :half] = square
        own_ref[j, half:] = tail
        for side in range(2):
            gram_copy(j, side).start()

    def two_steps(_, carry):
        u, z = split3(u_ref[...]), split3(z_ref[...])
        g = split3(growth(u, z, size))
        u_ref[...] = product(u, g)
        z_ref[...] = product(g, z)
        return carry

    make_gram(0)
    loops = ITERS // 2 - 2

    def analyse(j, carry):
        for side in range(2):
            gram_copy(j, side).wait_recv()
        full, right = unpack(own_ref[j] + 0.5 * (west_ref[j] + east_ref[j]), size)
        system = (size - 1.0) * identity_of(size) + full
        total = jnp.sum(jnp.sum(system * system, axis=0, keepdims=True), axis=1, keepdims=True)
        scale = jnp.sqrt(total + 1e-6)
        right_ref[...] = right
        scale_ref[...] = jnp.broadcast_to(scale, (1, LANES))
        u = system / scale
        g = growth(u, None, size)
        z_ref[...] = g
        u_ref[...] = product(split3(u), split3(g))
        lax.fori_loop(0, loops // 2, two_steps, 0)

        @pl.when(j + 1 < owned)
        def _():
            make_gram(j + 1)

        lax.fori_loop(loops // 2, loops, two_steps, 0)
        u, z = split3(u_ref[...]), split3(z_ref[...])
        inverse = product(split3(growth(u, z, size)), z) / jnp.sqrt(scale_ref[:, :1])
        pulled = jnp.sum(inverse * right_ref[...], axis=1, keepdims=True)
        shift = jnp.sum(inverse * pulled, axis=0, keepdims=True)
        weights = math.sqrt(size - 1.0) * inverse + shift
        states = got_ref[j]
        average = jnp.sum(states, axis=0, keepdims=True) / size
        w1, w2, _ = split3(weights)
        d1, d2, _ = split3(states - average)
        left = jnp.concatenate([w2, w1, w1], axis=1)
        right = jnp.concatenate([d1, d2, d1], axis=0)
        result_ref[j] = average + dot(left, right)
        for k in range(1, count):
            out_copy(j, k).start()
        out_ref[:, j * count + me, :] = result_ref[j, pl.ds(pl.multiple_of(me * rows, rows), rows)]
        return carry

    lax.fori_loop(0, owned, analyse, 0)

    def finish(j, carry):
        for k in range(1, count):
            in_copy(j, k).wait_send()
            out_copy(j, k).wait()
        for side in range(2):
            gram_copy(j, side).wait_send()
        return carry

    lax.fori_loop(0, owned, finish, 0)


def shards(members, obs_value, obs_precision, obs_index, obs_count):
    count, columns = lax.axis_size("member"), lax.axis_size("region")
    rows, tiles, width = members.shape
    owned = tiles // count
    size = count * rows
    packed = pltpu.VMEM((owned, size // 2 + 8, size), F32)
    whole = pl.BlockSpec(memory_space=pltpu.VMEM)
    table = obs_value.shape
    dma = pltpu.SemaphoreType.DMA
    out = pl.pallas_call(
        functools.partial(kernel, count, columns),
        in_specs=[pl.BlockSpec(memory_space=pltpu.HBM)] * 5,
        out_specs=whole,
        out_shape=jax.ShapeDtypeStruct((rows, tiles, width), F32),
        scratch_shapes=[
            pltpu.VMEM(table, F32),
            pltpu.VMEM(table, F32),
            pltpu.VMEM(table, jnp.int32),
            pltpu.SMEM(obs_count.shape, jnp.int32),
            pltpu.VMEM((owned, size, width), F32),
            packed, packed, packed,
            pltpu.VMEM((owned, size, width), F32),
            pltpu.VMEM((size, size), F32),
            pltpu.VMEM((size, size), F32),
            pltpu.VMEM((1, size), F32),
            pltpu.VMEM((1, LANES), F32),
            dma((owned,)),
            dma((4,)),
            pltpu.SemaphoreType.REGULAR,
            pltpu.SemaphoreType.REGULAR,
            dma((owned, count - 1)),
            dma((owned, count - 1)),
            dma((owned, 2)),
            dma((owned, 2)),
            dma((owned, count - 1)),
            dma((owned, count - 1)),
        ],
        compiler_params=pltpu.CompilerParams(
            collective_id=0, has_side_effects=True, vmem_limit_bytes=44 * 2**20
        ),
    )(*(
        pltpu.with_memory_space_constraint(a, pltpu.HBM)
        for a in (members, obs_value, obs_precision, obs_index, obs_count)
    ))
    return out


def solution(mesh):
    in_specs = (
        P("member", "region", None),
        P("region", None),
        P("region", None),
        P("region", None),
        P("region"),
    )
    return jax.shard_map(
        shards,
        mesh=mesh,
        in_specs=in_specs,
        out_specs=P("member", "region", None),
        check_vma=False,
    )
```

```python
import functools
import math

import jax
import jax.numpy as jnp
from jax import lax
from jax.experimental import pallas as pl
from jax.experimental.pallas import tpu as pltpu
from jax.sharding import PartitionSpec as P

ITERS = 12
LANES = 128
MESH = pl.DeviceIdType.MESH
F32 = jnp.float32
BF16 = jnp.bfloat16


def split3(x):
    a = x.astype(BF16)
    rest = x - a.astype(F32)
    b = rest.astype(BF16)
    return a, b, (rest - b.astype(F32)).astype(BF16)


def dot(a, b):
    return jnp.dot(a, b, preferred_element_type=F32)


def dot_nt(a, b):
    return lax.dot_general(a, b, (((1,), (1,)), ((), ())), preferred_element_type=F32)


def product(a, b):
    a1, a2, a3 = a
    b1, b2, b3 = b
    left = jnp.concatenate([a1, a3, a2, a1, a2, a1], axis=1)
    right = jnp.concatenate([b3, b1, b2, b2, b1, b1], axis=0)
    return dot(left, right)


def gram(states, places, exact, observed):
    size, width = states.shape
    half = size // 2
    groups = width // LANES
    slots = places.shape[1]

    high = lax.shift_right_logical(places, 7)
    low = lax.bitwise_and(places, LANES - 1)
    rows = lax.broadcasted_iota(jnp.int32, (groups, slots), 0) == high
    both = jnp.concatenate(
        [jnp.where(rows, exact, 0.0), jnp.where(rows, exact * observed, 0.0)], axis=0
    )
    one_hot = jnp.where(
        lax.broadcasted_iota(jnp.int32, (LANES, slots), 0) == low, 1.0, 0.0
    ).astype(BF16)
    e1, e2, e3 = split3(both)
    sums = dot_nt(e3, one_hot) + dot_nt(e2, one_hot) + dot_nt(e1, one_hot)
    c = jnp.concatenate([sums[i : i + 1] for i in range(groups)], axis=1)
    d = jnp.concatenate([sums[groups + i : groups + i + 1] for i in range(groups)], axis=1)

    average = jnp.sum(states, axis=0, keepdims=True) / size
    deviation = states - average
    s1, s2, s3 = split3(deviation * jnp.sqrt(c))
    cross = dot_nt(s1, s3) + dot_nt(s1, s2)
    own = (dot_nt(s2, s2) + (cross + cross.T)) + dot_nt(s1, s1)

    pulled = deviation * (d - c * average)
    folded = pulled[:, :LANES]
    for i in range(1, groups):
        folded = folded + pulled[:, i * LANES : (i + 1) * LANES]
    right = jnp.sum(folded.T, axis=0, keepdims=True)

    row = lax.broadcasted_iota(jnp.int32, (half, half), 0)
    col = lax.broadcasted_iota(jnp.int32, (half, half), 1)
    first, last = own[:half, :half], own[half:, half:]
    diagonal = jnp.sum(jnp.where(row == col, last, 0.0), axis=0, keepdims=True)
    square = jnp.concatenate([own[:half, half:], jnp.where(row <= col, first, last)], axis=1)
    tail = jnp.concatenate([right, jnp.concatenate([diagonal, diagonal], axis=1)], axis=0)
    return square, jnp.concatenate([tail, jnp.zeros((6, size), F32)], axis=0)


def unpack(packed, size):
    half = size // 2
    row = lax.broadcasted_iota(jnp.int32, (half, half), 0)
    col = lax.broadcasted_iota(jnp.int32, (half, half), 1)
    upper, mixed = packed[:half, :half], packed[:half, half:]
    right = packed[half : half + 1]
    diagonal = packed[half + 1 : half + 2, :half]
    turned = mixed.T
    first = jnp.where(row <= col, mixed, turned)
    last = jnp.where(row > col, mixed, turned)
    last = jnp.where(row == col, diagonal, last)
    full = jnp.concatenate(
        [
            jnp.concatenate([first, upper], axis=1),
            jnp.concatenate([upper.T, last], axis=1),
        ],
        axis=0,
    )
    return full, right


def identity_of(size):
    row = lax.broadcasted_iota(jnp.int32, (size, size), 0)
    col = lax.broadcasted_iota(jnp.int32, (size, size), 1)
    return jnp.where(row == col, 1.0, 0.0).astype(F32)


def growth(u, z, size):
    identity = identity_of(size)
    x = split3(u if z is None else product(z, u))
    plain = u if z is None else x[0].astype(F32) + x[1].astype(F32) + x[2].astype(F32)
    squared = product(x, x)
    inner = (1 / 16) * squared - (9 / 16) * plain
    outer = product(split3(squared), split3(inner))
    return (36 / 16) * identity - (39 / 16) * plain + (27 / 16) * squared + outer


def kernel(
    count, columns,
    x_hbm, value_hbm, precision_hbm, index_hbm, filled_hbm, out_ref,
    value_ref, precision_ref, index_ref, filled_ref, got_ref, own_ref, west_ref, east_ref, result_ref,
    u_ref, z_ref, right_ref, scale_ref,
    x_sem, table_sem, go_sem, open_sem, in_send, in_recv, gram_send, gram_recv, out_send, out_recv,
):
    me, column = lax.axis_index("member"), lax.axis_index("region")
    owned, size, width = got_ref.shape
    tiles = owned * count
    rows = size // count
    slots = index_ref.shape[1]
    half = size // 2

    def peer(k):
        return lax.rem(me + k, count)

    def own_copy(j):
        return pltpu.make_async_copy(
            x_hbm.at[:, j * count + me, :],
            got_ref.at[j, pl.ds(pl.multiple_of(me * rows, rows), rows)],
            x_sem.at[j],
        )

    tables = (
        (value_hbm, value_ref),
        (precision_hbm, precision_ref),
        (index_hbm, index_ref),
        (filled_hbm, filled_ref),
    )
    table_copies = [
        pltpu.make_async_copy(a, b, table_sem.at[i]) for i, (a, b) in enumerate(tables)
    ]

    beside = (lax.rem(column + 1, columns), lax.rem(column + columns - 1, columns))
    barrier = pltpu.get_barrier_semaphore()
    paired = count % 2 == 0
    first = lax.rem(me, 2) == 0
    partner = me + 1 - 2 * lax.rem(me, 2)

    def greet():
        for b in beside:
            pl.semaphore_signal(barrier, inc=1, device_id={"region": b}, device_id_type=MESH)

    def tell(semaphore):
        pl.semaphore_signal(
            semaphore, inc=1, device_id={"member": partner}, device_id_type=MESH
        )

    for k in range(1, count):
        pl.semaphore_signal(barrier, inc=1, device_id={"member": peer(k)}, device_id_type=MESH)
    if paired:

        @pl.when(first)
        def _():
            pl.semaphore_wait(barrier, count - 1)
            tell(go_sem)

        @pl.when(jnp.logical_not(first))
        def _():
            pl.semaphore_wait(go_sem, 1)

    else:
        greet()
        pl.semaphore_wait(barrier, count + 1)

    def meet_region():
        if paired:

            @pl.when(first)
            def _():
                pl.semaphore_wait(open_sem, 1)

            @pl.when(jnp.logical_not(first))
            def _():
                greet()
                pl.semaphore_wait(barrier, count + 1)
                tell(open_sem)

    def in_copy(j, k):
        return pltpu.make_async_remote_copy(
            src_ref=x_hbm.at[:, j * count + peer(k), :],
            dst_ref=got_ref.at[j, pl.ds(pl.multiple_of(me * rows, rows), rows)],
            send_sem=in_send.at[j, k - 1],
            recv_sem=in_recv.at[j, k - 1],
            device_id={"member": peer(k)},
            device_id_type=MESH,
        )

    def out_copy(j, k):
        return pltpu.make_async_remote_copy(
            src_ref=result_ref.at[j, pl.ds(pl.multiple_of(peer(k) * rows, rows), rows)],
            dst_ref=out_ref.at[:, j * count + me, :],
            send_sem=out_send.at[j, k - 1],
            recv_sem=out_recv.at[j, k - 1],
            device_id={"member": peer(k)},
            device_id_type=MESH,
        )

    def gram_copy(j, side):
        return pltpu.make_async_remote_copy(
            src_ref=own_ref.at[j],
            dst_ref=(west_ref, east_ref)[side].at[j],
            send_sem=gram_send.at[j, side],
            recv_sem=gram_recv.at[j, side],
            device_id={"region": beside[side]},
            device_id_type=MESH,
        )

    for j in range(owned):
        for k in range(1, count):
            in_copy(j, k).start()
    for j in range(owned):
        own_copy(j).start()
    for copy in table_copies:
        copy.start()
    for copy in table_copies:
        copy.wait()
    meet_region()

    def make_gram(j):
        own_copy(j).wait()
        for k in range(1, count):
            in_copy(j, k).wait_recv()
        t = j * count + me
        slot = lax.broadcasted_iota(jnp.int32, (1, slots), 1)
        exact = jnp.where(slot < filled_ref[t], precision_ref[pl.ds(t, 1), :], 0.0)
        square, tail = gram(
            got_ref[j], index_ref[pl.ds(t, 1), :], exact, value_ref[pl.ds(t, 1), :]
        )
        own_ref[j, :half] = square
        own_ref[j, half:] = tail
        for side in range(2):
            gram_copy(j, side).start()

    def two_steps(_, carry):
        u, z = split3(u_ref[...]), split3(z_ref[...])
        g = split3(growth(u, z, size))
        u_ref[...] = product(u, g)
        z_ref[...] = product(g, z)
        return carry

    make_gram(0)
    loops = ITERS // 2 - 2

    def analyse(j, carry):
        for side in range(2):
            gram_copy(j, side).wait_recv()
        full, right = unpack(own_ref[j] + 0.5 * (west_ref[j] + east_ref[j]), size)
        system = (size - 1.0) * identity_of(size) + full
        total = jnp.sum(jnp.sum(system * system, axis=0, keepdims=True), axis=1, keepdims=True)
        scale = jnp.sqrt(total + 1e-6)
        right_ref[...] = right
        scale_ref[...] = jnp.broadcast_to(scale, (1, LANES))
        u = system / scale
        g = growth(u, None, size)
        z_ref[...] = g
        u_ref[...] = product(split3(u), split3(g))
        lax.fori_loop(0, loops // 2, two_steps, 0)

        @pl.when(j + 1 < owned)
        def _():
            make_gram(j + 1)

        lax.fori_loop(loops // 2, loops, two_steps, 0)
        u, z = split3(u_ref[...]), split3(z_ref[...])
        inverse = product(split3(growth(u, z, size)), z) / jnp.sqrt(scale_ref[:, :1])
        pulled = jnp.sum(inverse * right_ref[...], axis=1, keepdims=True)
        shift = jnp.sum(inverse * pulled, axis=0, keepdims=True)
        weights = math.sqrt(size - 1.0) * inverse + shift
        states = got_ref[j]
        average = jnp.sum(states, axis=0, keepdims=True) / size
        w1, w2, _ = split3(weights)
        d1, d2, _ = split3(states - average)
        left = jnp.concatenate([w2, w1, w1], axis=1)
        right = jnp.concatenate([d1, d2, d1], axis=0)
        result_ref[j] = average + dot(left, right)
        out_ref[:, j * count + me, :] = result_ref[j, pl.ds(pl.multiple_of(me * rows, rows), rows)]
        for k in range(1, count):
            out_copy(j, k).start()
        return carry

    lax.fori_loop(0, owned, analyse, 0)

    def finish(j, carry):
        for k in range(1, count):
            in_copy(j, k).wait_send()
            out_copy(j, k).wait()
        for side in range(2):
            gram_copy(j, side).wait_send()
        return carry

    lax.fori_loop(0, owned, finish, 0)


def shards(members, obs_value, obs_precision, obs_index, obs_count):
    count, columns = lax.axis_size("member"), lax.axis_size("region")
    rows, tiles, width = members.shape
    owned = tiles // count
    size = count * rows
    packed = pltpu.VMEM((owned, size // 2 + 8, size), F32)
    whole = pl.BlockSpec(memory_space=pltpu.VMEM)
    table = obs_value.shape
    dma = pltpu.SemaphoreType.DMA
    out = pl.pallas_call(
        functools.partial(kernel, count, columns),
        in_specs=[pl.BlockSpec(memory_space=pltpu.HBM)] * 5,
        out_specs=whole,
        out_shape=jax.ShapeDtypeStruct((rows, tiles, width), F32),
        scratch_shapes=[
            pltpu.VMEM(table, F32),
            pltpu.VMEM(table, F32),
            pltpu.VMEM(table, jnp.int32),
            pltpu.SMEM(obs_count.shape, jnp.int32),
            pltpu.VMEM((owned, size, width), F32),
            packed, packed, packed,
            pltpu.VMEM((owned, size, width), F32),
            pltpu.VMEM((size, size), F32),
            pltpu.VMEM((size, size), F32),
            pltpu.VMEM((1, size), F32),
            pltpu.VMEM((1, LANES), F32),
            dma((owned,)),
            dma((4,)),
            pltpu.SemaphoreType.REGULAR,
            pltpu.SemaphoreType.REGULAR,
            dma((owned, count - 1)),
            dma((owned, count - 1)),
            dma((owned, 2)),
            dma((owned, 2)),
            dma((owned, count - 1)),
            dma((owned, count - 1)),
        ],
        compiler_params=pltpu.CompilerParams(
            collective_id=0, has_side_effects=True, vmem_limit_bytes=44 * 2**20
        ),
    )(*(
        pltpu.with_memory_space_constraint(a, pltpu.HBM)
        for a in (members, obs_value, obs_precision, obs_index, obs_count)
    ))
    return out


def solution(mesh):
    in_specs = (
        P("member", "region", None),
        P("region", None),
        P("region", None),
        P("region", None),
        P("region"),
    )
    return jax.shard_map(
        shards,
        mesh=mesh,
        in_specs=in_specs,
        out_specs=P("member", "region", None),
        check_vma=False,
    )
```

```python
import functools
import math

import jax
import jax.numpy as jnp
from jax import lax
from jax.experimental import pallas as pl
from jax.experimental.pallas import tpu as pltpu
from jax.sharding import PartitionSpec as P

ITERS = 12
LANES = 128
MESH = pl.DeviceIdType.MESH
F32 = jnp.float32
BF16 = jnp.bfloat16


def split3(x):
    a = x.astype(BF16)
    rest = x - a.astype(F32)
    b = rest.astype(BF16)
    return a, b, (rest - b.astype(F32)).astype(BF16)


def dot(a, b):
    return jnp.dot(a, b, preferred_element_type=F32)


def dot_nt(a, b):
    return lax.dot_general(a, b, (((1,), (1,)), ((), ())), preferred_element_type=F32)


def product(a, b):
    a1, a2, a3 = a
    b1, b2, b3 = b
    left = jnp.concatenate([a1, a3, a2, a1, a2, a1], axis=1)
    right = jnp.concatenate([b3, b1, b2, b2, b1, b1], axis=0)
    return dot(left, right)


def gram(states, places, exact, observed):
    size, width = states.shape
    half = size // 2
    groups = width // LANES
    slots = places.shape[1]

    high = lax.shift_right_logical(places, 7)
    low = lax.bitwise_and(places, LANES - 1)
    rows = lax.broadcasted_iota(jnp.int32, (groups, slots), 0) == high
    both = jnp.concatenate(
        [jnp.where(rows, exact, 0.0), jnp.where(rows, exact * observed, 0.0)], axis=0
    )
    one_hot = jnp.where(
        lax.broadcasted_iota(jnp.int32, (LANES, slots), 0) == low, 1.0, 0.0
    ).astype(BF16)
    e1, e2, e3 = split3(both)
    sums = dot_nt(e3, one_hot) + dot_nt(e2, one_hot) + dot_nt(e1, one_hot)
    c = jnp.concatenate([sums[i : i + 1] for i in range(groups)], axis=1)
    d = jnp.concatenate([sums[groups + i : groups + i + 1] for i in range(groups)], axis=1)

    average = jnp.sum(states, axis=0, keepdims=True) / size
    deviation = states - average
    s1, s2, s3 = split3(deviation * jnp.sqrt(c))
    cross = dot_nt(s1, s3) + dot_nt(s1, s2)
    own = (dot_nt(s2, s2) + (cross + cross.T)) + dot_nt(s1, s1)

    pulled = deviation * (d - c * average)
    folded = pulled[:, :LANES]
    for i in range(1, groups):
        folded = folded + pulled[:, i * LANES : (i + 1) * LANES]
    right = jnp.sum(folded.T, axis=0, keepdims=True)

    row = lax.broadcasted_iota(jnp.int32, (half, half), 0)
    col = lax.broadcasted_iota(jnp.int32, (half, half), 1)
    first, last = own[:half, :half], own[half:, half:]
    diagonal = jnp.sum(jnp.where(row == col, last, 0.0), axis=0, keepdims=True)
    square = jnp.concatenate([own[:half, half:], jnp.where(row <= col, first, last)], axis=1)
    tail = jnp.concatenate([right, jnp.concatenate([diagonal, diagonal], axis=1)], axis=0)
    return square, jnp.concatenate([tail, jnp.zeros((6, size), F32)], axis=0)


def unpack(packed, size):
    half = size // 2
    row = lax.broadcasted_iota(jnp.int32, (half, half), 0)
    col = lax.broadcasted_iota(jnp.int32, (half, half), 1)
    upper, mixed = packed[:half, :half], packed[:half, half:]
    right = packed[half : half + 1]
    diagonal = packed[half + 1 : half + 2, :half]
    turned = mixed.T
    first = jnp.where(row <= col, mixed, turned)
    last = jnp.where(row > col, mixed, turned)
    last = jnp.where(row == col, diagonal, last)
    full = jnp.concatenate(
        [
            jnp.concatenate([first, upper], axis=1),
            jnp.concatenate([upper.T, last], axis=1),
        ],
        axis=0,
    )
    return full, right


def identity_of(size):
    row = lax.broadcasted_iota(jnp.int32, (size, size), 0)
    col = lax.broadcasted_iota(jnp.int32, (size, size), 1)
    return jnp.where(row == col, 1.0, 0.0).astype(F32)


def growth(u, z, size):
    identity = identity_of(size)
    x = split3(u if z is None else product(z, u))
    plain = u if z is None else x[0].astype(F32) + x[1].astype(F32) + x[2].astype(F32)
    squared = product(x, x)
    inner = (1 / 16) * squared - (9 / 16) * plain
    outer = product(split3(squared), split3(inner))
    return (36 / 16) * identity - (39 / 16) * plain + (27 / 16) * squared + outer


def kernel(
    count, columns,
    x_hbm, value_hbm, precision_hbm, index_hbm, filled_hbm, out_ref,
    value_ref, precision_ref, index_ref, filled_ref, got_ref, own_ref, west_ref, east_ref, result_ref,
    u_ref, z_ref, right_ref, scale_ref,
    x_sem, table_sem, go_sem, open_sem, in_send, in_recv, gram_send, gram_recv, out_send, out_recv,
):
    me, column = lax.axis_index("member"), lax.axis_index("region")
    owned, size, width = got_ref.shape
    tiles = owned * count
    rows = size // count
    slots = index_ref.shape[1]
    half = size // 2

    def peer(k):
        return lax.rem(me + k, count)

    def own_copy(j):
        return pltpu.make_async_copy(
            x_hbm.at[:, j * count + me, :],
            got_ref.at[j, pl.ds(pl.multiple_of(me * rows, rows), rows)],
            x_sem.at[j],
        )

    tables = (
        (value_hbm, value_ref),
        (precision_hbm, precision_ref),
        (index_hbm, index_ref),
        (filled_hbm, filled_ref),
    )
    table_copies = [
        pltpu.make_async_copy(a, b, table_sem.at[i]) for i, (a, b) in enumerate(tables)
    ]

    beside = (lax.rem(column + 1, columns), lax.rem(column + columns - 1, columns))
    barrier = pltpu.get_barrier_semaphore()
    paired = count % 2 == 0
    first = lax.rem(me, 2) == 0
    partner = me + 1 - 2 * lax.rem(me, 2)

    def greet():
        for b in beside:
            pl.semaphore_signal(barrier, inc=1, device_id={"region": b}, device_id_type=MESH)

    def tell(semaphore):
        pl.semaphore_signal(
            semaphore, inc=1, device_id={"member": partner}, device_id_type=MESH
        )

    for k in range(1, count):
        pl.semaphore_signal(barrier, inc=1, device_id={"member": peer(k)}, device_id_type=MESH)
    if paired:

        @pl.when(first)
        def _():
            pl.semaphore_wait(barrier, count - 1)
            tell(go_sem)

        @pl.when(jnp.logical_not(first))
        def _():
            pl.semaphore_wait(go_sem, 1)

    else:
        greet()
        pl.semaphore_wait(barrier, count + 1)

    def meet_region():
        if paired:

            @pl.when(first)
            def _():
                pl.semaphore_wait(open_sem, 1)

            @pl.when(jnp.logical_not(first))
            def _():
                greet()
                pl.semaphore_wait(barrier, count + 1)
                tell(open_sem)

    def in_copy(j, k):
        return pltpu.make_async_remote_copy(
            src_ref=x_hbm.at[:, j * count + peer(k), :],
            dst_ref=got_ref.at[j, pl.ds(pl.multiple_of(me * rows, rows), rows)],
            send_sem=in_send.at[j, k - 1],
            recv_sem=in_recv.at[j, k - 1],
            device_id={"member": peer(k)},
            device_id_type=MESH,
        )

    def out_copy(j, k):
        return pltpu.make_async_remote_copy(
            src_ref=result_ref.at[j, pl.ds(pl.multiple_of(peer(k) * rows, rows), rows)],
            dst_ref=out_ref.at[:, j * count + me, :],
            send_sem=out_send.at[j, k - 1],
            recv_sem=out_recv.at[j, k - 1],
            device_id={"member": peer(k)},
            device_id_type=MESH,
        )

    def gram_copy(j, side):
        return pltpu.make_async_remote_copy(
            src_ref=own_ref.at[j],
            dst_ref=(west_ref, east_ref)[side].at[j],
            send_sem=gram_send.at[j, side],
            recv_sem=gram_recv.at[j, side],
            device_id={"region": beside[side]},
            device_id_type=MESH,
        )

    farthest_first = sorted(range(1, count), key=lambda k: abs(2 * k - count))
    for j in range(owned):
        for k in farthest_first:
            in_copy(j, k).start()
    for j in range(owned):
        own_copy(j).start()
    for copy in table_copies:
        copy.start()
    for copy in table_copies:
        copy.wait()
    meet_region()

    def make_gram(j):
        own_copy(j).wait()
        for k in range(1, count):
            in_copy(j, k).wait_recv()
        t = j * count + me
        slot = lax.broadcasted_iota(jnp.int32, (1, slots), 1)
        exact = jnp.where(slot < filled_ref[t], precision_ref[pl.ds(t, 1), :], 0.0)
        square, tail = gram(
            got_ref[j], index_ref[pl.ds(t, 1), :], exact, value_ref[pl.ds(t, 1), :]
        )
        own_ref[j, :half] = square
        own_ref[j, half:] = tail
        for side in range(2):
            gram_copy(j, side).start()

    def two_steps(_, carry):
        u, z = split3(u_ref[...]), split3(z_ref[...])
        g = split3(growth(u, z, size))
        u_ref[...] = product(u, g)
        z_ref[...] = product(g, z)
        return carry

    make_gram(0)
    loops = ITERS // 2 - 2

    def analyse(j, carry):
        for side in range(2):
            gram_copy(j, side).wait_recv()
        full, right = unpack(own_ref[j] + 0.5 * (west_ref[j] + east_ref[j]), size)
        system = (size - 1.0) * identity_of(size) + full
        total = jnp.sum(jnp.sum(system * system, axis=0, keepdims=True), axis=1, keepdims=True)
        scale = jnp.sqrt(total + 1e-6)
        right_ref[...] = right
        scale_ref[...] = jnp.broadcast_to(scale, (1, LANES))
        u = system / scale
        g = growth(u, None, size)
        z_ref[...] = g
        u_ref[...] = product(split3(u), split3(g))
        lax.fori_loop(0, loops // 2, two_steps, 0)

        @pl.when(j + 1 < owned)
        def _():
            make_gram(j + 1)

        lax.fori_loop(loops // 2, loops, two_steps, 0)
        u, z = split3(u_ref[...]), split3(z_ref[...])
        inverse = product(split3(growth(u, z, size)), z) / jnp.sqrt(scale_ref[:, :1])
        pulled = jnp.sum(inverse * right_ref[...], axis=1, keepdims=True)
        shift = jnp.sum(inverse * pulled, axis=0, keepdims=True)
        weights = math.sqrt(size - 1.0) * inverse + shift
        states = got_ref[j]
        average = jnp.sum(states, axis=0, keepdims=True) / size
        w1, w2, _ = split3(weights)
        d1, d2, _ = split3(states - average)
        left = jnp.concatenate([w2, w1, w1], axis=1)
        right = jnp.concatenate([d1, d2, d1], axis=0)
        result_ref[j] = average + dot(left, right)
        out_ref[:, j * count + me, :] = result_ref[j, pl.ds(pl.multiple_of(me * rows, rows), rows)]
        for k in range(1, count):
            out_copy(j, k).start()
        return carry

    lax.fori_loop(0, owned, analyse, 0)

    def finish(j, carry):
        for k in range(1, count):
            in_copy(j, k).wait_send()
            out_copy(j, k).wait()
        for side in range(2):
            gram_copy(j, side).wait_send()
        return carry

    lax.fori_loop(0, owned, finish, 0)


def flush_kernel(held_ref, out_hbm, sem):
    copy = pltpu.make_async_copy(held_ref, out_hbm, sem)
    copy.start()
    copy.wait()


def flush(held):
    return pl.pallas_call(
        flush_kernel,
        in_specs=[pl.BlockSpec(memory_space=pltpu.VMEM)],
        out_specs=pl.BlockSpec(memory_space=pltpu.HBM),
        out_shape=jax.ShapeDtypeStruct(held.shape, held.dtype),
        scratch_shapes=[pltpu.SemaphoreType.DMA],
        cost_estimate=pl.CostEstimate(
            flops=0, bytes_accessed=held.size * 4, transcendentals=0
        ),
        compiler_params=pltpu.CompilerParams(vmem_limit_bytes=16 * 2**20),
    )(held)


def shards(members, obs_value, obs_precision, obs_index, obs_count):
    count, columns = lax.axis_size("member"), lax.axis_size("region")
    rows, tiles, width = members.shape
    owned = tiles // count
    size = count * rows
    packed = pltpu.VMEM((owned, size // 2 + 8, size), F32)
    whole = pl.BlockSpec(memory_space=pltpu.VMEM)
    table = obs_value.shape
    dma = pltpu.SemaphoreType.DMA
    out = pl.pallas_call(
        functools.partial(kernel, count, columns),
        in_specs=[pl.BlockSpec(memory_space=pltpu.HBM)] * 5,
        out_specs=whole,
        out_shape=jax.ShapeDtypeStruct((rows, tiles, width), F32),
        scratch_shapes=[
            pltpu.VMEM(table, F32),
            pltpu.VMEM(table, F32),
            pltpu.VMEM(table, jnp.int32),
            pltpu.SMEM(obs_count.shape, jnp.int32),
            pltpu.VMEM((owned, size, width), F32),
            packed, packed, packed,
            pltpu.VMEM((owned, size, width), F32),
            pltpu.VMEM((size, size), F32),
            pltpu.VMEM((size, size), F32),
            pltpu.VMEM((1, size), F32),
            pltpu.VMEM((1, LANES), F32),
            dma((owned,)),
            dma((4,)),
            pltpu.SemaphoreType.REGULAR,
            pltpu.SemaphoreType.REGULAR,
            dma((owned, count - 1)),
            dma((owned, count - 1)),
            dma((owned, 2)),
            dma((owned, 2)),
            dma((owned, count - 1)),
            dma((owned, count - 1)),
        ],
        compiler_params=pltpu.CompilerParams(
            collective_id=0, has_side_effects=True, vmem_limit_bytes=44 * 2**20
        ),
    )(*(
        pltpu.with_memory_space_constraint(a, pltpu.HBM)
        for a in (members, obs_value, obs_precision, obs_index, obs_count)
    ))
    return flush(out)


def solution(mesh):
    in_specs = (
        P("member", "region", None),
        P("region", None),
        P("region", None),
        P("region", None),
        P("region"),
    )
    return jax.shard_map(
        shards,
        mesh=mesh,
        in_specs=in_specs,
        out_specs=P("member", "region", None),
        check_vma=False,
    )
```

```python
import functools
import math

import jax
import jax.numpy as jnp
from jax import lax
from jax.experimental import pallas as pl
from jax.experimental.pallas import tpu as pltpu
from jax.sharding import PartitionSpec as P

ITERS = 12
LANES = 128
MESH = pl.DeviceIdType.MESH
F32 = jnp.float32
BF16 = jnp.bfloat16


def split3(x):
    a = x.astype(BF16)
    rest = x - a.astype(F32)
    b = rest.astype(BF16)
    return a, b, (rest - b.astype(F32)).astype(BF16)


def dot(a, b):
    return jnp.dot(a, b, preferred_element_type=F32)


def dot_nt(a, b):
    return lax.dot_general(a, b, (((1,), (1,)), ((), ())), preferred_element_type=F32)


def product(a, b):
    a1, a2, a3 = a
    b1, b2, b3 = b
    left = jnp.concatenate([a1, a3, a2, a1, a2, a1], axis=1)
    right = jnp.concatenate([b3, b1, b2, b2, b1, b1], axis=0)
    return dot(left, right)


def gram(states, places, exact, observed):
    size, width = states.shape
    half = size // 2
    groups = width // LANES
    slots = places.shape[1]

    high = lax.shift_right_logical(places, 7)
    low = lax.bitwise_and(places, LANES - 1)
    rows = lax.broadcasted_iota(jnp.int32, (groups, slots), 0) == high
    both = jnp.concatenate(
        [jnp.where(rows, exact, 0.0), jnp.where(rows, exact * observed, 0.0)], axis=0
    )
    one_hot = jnp.where(
        lax.broadcasted_iota(jnp.int32, (LANES, slots), 0) == low, 1.0, 0.0
    ).astype(BF16)
    e1, e2, e3 = split3(both)
    sums = dot_nt(e3, one_hot) + dot_nt(e2, one_hot) + dot_nt(e1, one_hot)
    c = jnp.concatenate([sums[i : i + 1] for i in range(groups)], axis=1)
    d = jnp.concatenate([sums[groups + i : groups + i + 1] for i in range(groups)], axis=1)

    average = jnp.sum(states, axis=0, keepdims=True) / size
    deviation = states - average
    s1, s2, s3 = split3(deviation * jnp.sqrt(c))
    cross = dot_nt(s1, s3) + dot_nt(s1, s2)
    own = (dot_nt(s2, s2) + (cross + cross.T)) + dot_nt(s1, s1)

    pulled = deviation * (d - c * average)
    folded = pulled[:, :LANES]
    for i in range(1, groups):
        folded = folded + pulled[:, i * LANES : (i + 1) * LANES]
    right = jnp.sum(folded.T, axis=0, keepdims=True)

    row = lax.broadcasted_iota(jnp.int32, (half, half), 0)
    col = lax.broadcasted_iota(jnp.int32, (half, half), 1)
    first, last = own[:half, :half], own[half:, half:]
    diagonal = jnp.sum(jnp.where(row == col, last, 0.0), axis=0, keepdims=True)
    square = jnp.concatenate([own[:half, half:], jnp.where(row <= col, first, last)], axis=1)
    tail = jnp.concatenate([right, jnp.concatenate([diagonal, diagonal], axis=1)], axis=0)
    return square, jnp.concatenate([tail, jnp.zeros((6, size), F32)], axis=0)


def unpack(packed, size):
    half = size // 2
    row = lax.broadcasted_iota(jnp.int32, (half, half), 0)
    col = lax.broadcasted_iota(jnp.int32, (half, half), 1)
    upper, mixed = packed[:half, :half], packed[:half, half:]
    right = packed[half : half + 1]
    diagonal = packed[half + 1 : half + 2, :half]
    turned = mixed.T
    first = jnp.where(row <= col, mixed, turned)
    last = jnp.where(row > col, mixed, turned)
    last = jnp.where(row == col, diagonal, last)
    full = jnp.concatenate(
        [
            jnp.concatenate([first, upper], axis=1),
            jnp.concatenate([upper.T, last], axis=1),
        ],
        axis=0,
    )
    return full, right


def identity_of(size):
    row = lax.broadcasted_iota(jnp.int32, (size, size), 0)
    col = lax.broadcasted_iota(jnp.int32, (size, size), 1)
    return jnp.where(row == col, 1.0, 0.0).astype(F32)


def growth(u, z, size):
    identity = identity_of(size)
    x = split3(u if z is None else product(z, u))
    plain = u if z is None else x[0].astype(F32) + x[1].astype(F32) + x[2].astype(F32)
    squared = product(x, x)
    inner = (1 / 16) * squared - (9 / 16) * plain
    outer = product(split3(squared), split3(inner))
    return (36 / 16) * identity - (39 / 16) * plain + (27 / 16) * squared + outer


def kernel(
    count, columns,
    x_hbm, value_hbm, precision_hbm, index_hbm, filled_hbm, out_ref,
    value_ref, precision_ref, index_ref, filled_ref, got_ref, own_ref, west_ref, east_ref, result_ref,
    u_ref, z_ref, right_ref, scale_ref,
    x_sem, table_sem, go_sem, open_sem, in_send, in_recv, gram_send, gram_recv, out_send, out_recv,
):
    me, column = lax.axis_index("member"), lax.axis_index("region")
    owned, size, width = got_ref.shape
    tiles = owned * count
    rows = size // count
    slots = index_ref.shape[1]
    half = size // 2

    def peer(k):
        return lax.rem(me + k, count)

    def own_copy(j):
        return pltpu.make_async_copy(
            x_hbm.at[:, j * count + me, :],
            got_ref.at[j, pl.ds(pl.multiple_of(me * rows, rows), rows)],
            x_sem.at[j],
        )

    tables = (
        (value_hbm, value_ref),
        (precision_hbm, precision_ref),
        (index_hbm, index_ref),
        (filled_hbm, filled_ref),
    )
    table_copies = [
        pltpu.make_async_copy(a, b, table_sem.at[i]) for i, (a, b) in enumerate(tables)
    ]

    beside = (lax.rem(column + 1, columns), lax.rem(column + columns - 1, columns))
    barrier = pltpu.get_barrier_semaphore()
    paired = count % 2 == 0
    first = lax.rem(me, 2) == 0
    partner = me + 1 - 2 * lax.rem(me, 2)

    def greet():
        for b in beside:
            pl.semaphore_signal(barrier, inc=1, device_id={"region": b}, device_id_type=MESH)

    def tell(semaphore):
        pl.semaphore_signal(
            semaphore, inc=1, device_id={"member": partner}, device_id_type=MESH
        )

    for k in range(1, count):
        pl.semaphore_signal(barrier, inc=1, device_id={"member": peer(k)}, device_id_type=MESH)
    if paired:

        @pl.when(first)
        def _():
            pl.semaphore_wait(barrier, count - 1)
            tell(go_sem)

        @pl.when(jnp.logical_not(first))
        def _():
            pl.semaphore_wait(go_sem, 1)

    else:
        greet()
        pl.semaphore_wait(barrier, count + 1)

    def meet_region():
        if paired:

            @pl.when(first)
            def _():
                pl.semaphore_wait(open_sem, 1)

            @pl.when(jnp.logical_not(first))
            def _():
                greet()
                pl.semaphore_wait(barrier, count + 1)
                tell(open_sem)

    def in_copy(j, k):
        return pltpu.make_async_remote_copy(
            src_ref=x_hbm.at[:, j * count + peer(k), :],
            dst_ref=got_ref.at[j, pl.ds(pl.multiple_of(me * rows, rows), rows)],
            send_sem=in_send.at[j, k - 1],
            recv_sem=in_recv.at[j, k - 1],
            device_id={"member": peer(k)},
            device_id_type=MESH,
        )

    def out_copy(j, k):
        return pltpu.make_async_remote_copy(
            src_ref=result_ref.at[j, pl.ds(pl.multiple_of(peer(k) * rows, rows), rows)],
            dst_ref=out_ref.at[:, j * count + me, :],
            send_sem=out_send.at[j, k - 1],
            recv_sem=out_recv.at[j, k - 1],
            device_id={"member": peer(k)},
            device_id_type=MESH,
        )

    def gram_copy(j, side):
        return pltpu.make_async_remote_copy(
            src_ref=own_ref.at[j],
            dst_ref=(west_ref, east_ref)[side].at[j],
            send_sem=gram_send.at[j, side],
            recv_sem=gram_recv.at[j, side],
            device_id={"region": beside[side]},
            device_id_type=MESH,
        )

    for j in range(owned):
        for k in range(1, count):
            in_copy(j, k).start()
    for j in range(owned):
        own_copy(j).start()
    for copy in table_copies:
        copy.start()
    for copy in table_copies:
        copy.wait()
    meet_region()

    def make_gram(j):
        own_copy(j).wait()
        for k in range(1, count):
            in_copy(j, k).wait_recv()
        t = j * count + me
        slot = lax.broadcasted_iota(jnp.int32, (1, slots), 1)
        exact = jnp.where(slot < filled_ref[t], precision_ref[pl.ds(t, 1), :], 0.0)
        square, tail = gram(
            got_ref[j], index_ref[pl.ds(t, 1), :], exact, value_ref[pl.ds(t, 1), :]
        )
        own_ref[j, :half] = square
        own_ref[j, half:] = tail
        for side in range(2):
            gram_copy(j, side).start()

    def two_steps(_, carry):
        u, z = split3(u_ref[...]), split3(z_ref[...])
        g = split3(growth(u, z, size))
        u_ref[...] = product(u, g)
        z_ref[...] = product(g, z)
        return carry

    make_gram(0)
    loops = ITERS // 2 - 2

    def analyse(j, carry):
        for side in range(2):
            gram_copy(j, side).wait_recv()
        full, right = unpack(own_ref[j] + 0.5 * (west_ref[j] + east_ref[j]), size)
        system = (size - 1.0) * identity_of(size) + full
        total = jnp.sum(jnp.sum(system * system, axis=0, keepdims=True), axis=1, keepdims=True)
        scale = jnp.sqrt(total + 1e-6)
        right_ref[...] = right
        scale_ref[...] = jnp.broadcast_to(scale, (1, LANES))
        u = system / scale
        g = growth(u, None, size)
        z_ref[...] = g
        u_ref[...] = product(split3(u), split3(g))
        lax.fori_loop(0, loops // 2, two_steps, 0)

        @pl.when(j + 1 < owned)
        def _():
            make_gram(j + 1)

        lax.fori_loop(loops // 2, loops, two_steps, 0)
        u, z = split3(u_ref[...]), split3(z_ref[...])
        inverse = product(split3(growth(u, z, size)), z) / jnp.sqrt(scale_ref[:, :1])
        pulled = jnp.sum(inverse * right_ref[...], axis=1, keepdims=True)
        shift = jnp.sum(inverse * pulled, axis=0, keepdims=True)
        weights = math.sqrt(size - 1.0) * inverse + shift
        states = got_ref[j]
        average = jnp.sum(states, axis=0, keepdims=True) / size
        w1, w2, _ = split3(weights)
        d1, d2, _ = split3(states - average)
        left = jnp.concatenate([w2, w1, w1], axis=1)
        right = jnp.concatenate([d1, d2, d1], axis=0)
        result_ref[j] = average + dot(left, right)
        out_ref[:, j * count + me, :] = result_ref[j, pl.ds(pl.multiple_of(me * rows, rows), rows)]
        for k in range(1, count):
            out_copy(j, k).start()
        return carry

    lax.fori_loop(0, owned, analyse, 0)

    def finish(j, carry):
        for k in range(1, count):
            in_copy(j, k).wait_send()
            out_copy(j, k).wait()
        for side in range(2):
            gram_copy(j, side).wait_send()
        return carry

    lax.fori_loop(0, owned, finish, 0)


def flush_kernel(held_ref, out_hbm, sem):
    copy = pltpu.make_async_copy(held_ref, out_hbm, sem)
    copy.start()
    copy.wait()


def flush(held):
    return pl.pallas_call(
        flush_kernel,
        in_specs=[pl.BlockSpec(memory_space=pltpu.VMEM)],
        out_specs=pl.BlockSpec(memory_space=pltpu.HBM),
        out_shape=jax.ShapeDtypeStruct(held.shape, held.dtype),
        scratch_shapes=[pltpu.SemaphoreType.DMA],
        cost_estimate=pl.CostEstimate(
            flops=0, bytes_accessed=held.size * 4, transcendentals=0
        ),
        compiler_params=pltpu.CompilerParams(vmem_limit_bytes=16 * 2**20),
    )(held)


def shards(members, obs_value, obs_precision, obs_index, obs_count):
    count, columns = lax.axis_size("member"), lax.axis_size("region")
    rows, tiles, width = members.shape
    owned = tiles // count
    size = count * rows
    packed = pltpu.VMEM((owned, size // 2 + 8, size), F32)
    whole = pl.BlockSpec(memory_space=pltpu.VMEM)
    table = obs_value.shape
    dma = pltpu.SemaphoreType.DMA
    out = pl.pallas_call(
        functools.partial(kernel, count, columns),
        in_specs=[pl.BlockSpec(memory_space=pltpu.HBM)] * 5,
        out_specs=whole,
        out_shape=jax.ShapeDtypeStruct((rows, tiles, width), F32),
        scratch_shapes=[
            pltpu.VMEM(table, F32),
            pltpu.VMEM(table, F32),
            pltpu.VMEM(table, jnp.int32),
            pltpu.SMEM(obs_count.shape, jnp.int32),
            pltpu.VMEM((owned, size, width), F32),
            packed, packed, packed,
            pltpu.VMEM((owned, size, width), F32),
            pltpu.VMEM((size, size), F32),
            pltpu.VMEM((size, size), F32),
            pltpu.VMEM((1, size), F32),
            pltpu.VMEM((1, LANES), F32),
            dma((owned,)),
            dma((4,)),
            pltpu.SemaphoreType.REGULAR,
            pltpu.SemaphoreType.REGULAR,
            dma((owned, count - 1)),
            dma((owned, count - 1)),
            dma((owned, 2)),
            dma((owned, 2)),
            dma((owned, count - 1)),
            dma((owned, count - 1)),
        ],
        compiler_params=pltpu.CompilerParams(
            collective_id=0, has_side_effects=True, vmem_limit_bytes=44 * 2**20
        ),
    )(*(
        pltpu.with_memory_space_constraint(a, pltpu.HBM)
        for a in (members, obs_value, obs_precision, obs_index, obs_count)
    ))
    return flush(out)


def solution(mesh):
    in_specs = (
        P("member", "region", None),
        P("region", None),
        P("region", None),
        P("region", None),
        P("region"),
    )
    return jax.shard_map(
        shards,
        mesh=mesh,
        in_specs=in_specs,
        out_specs=P("member", "region", None),
        check_vma=False,
    )
```
